512 devices in a mesh: dp: 64 (over x, z, core), mp: 8 (over y).
Axes of the slice: x: 4, y: 8, z: 8, core: 2. Of those that a mesh axis runs over, the one named last changes fastest.
Arguments:
- node_feats: bfloat16 [256, 131072], P('mp', 'dp'), may hold values from -6 to 6
- proj_weight: bfloat16 [256, 256], P('mp'), may hold values from -0.375 to 0.375
- att_src: float32 [256], P('mp'), may hold values from -32 to 32
- att_dst: float32 [256], P('mp'), may hold values from -32 to 32
- out_bias: float32 [256], P('mp'), may hold values from -3 to 3
- tile_rows: int32 [2048], P('dp'), may hold values from 0 to 1023, as said below
- tile_cols: int32 [2048], P('dp'), may hold values from 0 to 1023, as said below
- tile_masks: int32 [2048, 4, 128], P('dp'), may hold values from -2147483648 to 2147483646
Outputs:
- node_out: bfloat16 [256, 131072], P('mp', 'dp')
The draws below stay inside these ranges and needn't reach their ends.
Inputs may be any that keep to these rules, and one draw needn't show every extreme that they name: `tile_rows`: block b holds nodes 128 b to 128 b + 127 and belongs to index b // 16 of dp. Among the 32 tiles of one index of dp, no owner's blocks are named more than 2 times; on every index one owner's blocks are named exactly 2 times. `tile_cols`: the same bound holds for source blocks: among the 32 tiles of one index of dp, no owner's blocks are named more than 2 times, and one owner's exactly 2 times on every index.
All inputs are finite; a program needn't handle non-finite values.
Results may differ from the reference program's by a relative error of at most 0.0034.
Values may be sent and summed in bfloat16 or wider, within the bound.
A program may use at most 64 MiB of HBM per device.

```python
import jax
import jax.numpy as jnp
from jax import lax

FIN = 256
HEADS = 8
HD = 32
TILE = 128
TILES_DEV = 32
NODES = 131072
BLK_DEV = 16
NBLK = 1024
TILES = 2048
CAP = 2
N_DP = 64


def tile_blocks(key, salt):
    base_key = jax.random.fold_in(key, salt)
    hub_owner = jax.random.randint(jax.random.fold_in(base_key, 7), (), 0, N_DP)

    def device_tiles(device):
        device_key = jax.random.fold_in(base_key, device)
        key_rest, key_shift, key_local, key_order = jax.random.split(device_key, 4)
        rest_slots = CAP + jax.random.permutation(key_rest, N_DP * CAP - CAP)[:TILES_DEV - CAP]
        position = jnp.concatenate([jnp.arange(CAP, dtype=jnp.int32), rest_slots.astype(jnp.int32)])
        shifts = jnp.concatenate([jnp.zeros((1,), jnp.int32), 1 + jax.random.permutation(key_shift, N_DP - 1).astype(jnp.int32)])
        owners = (hub_owner + shifts[position // CAP]) % N_DP
        local_block = jax.random.randint(key_local, (TILES_DEV,), 0, BLK_DEV)
        blocks = owners * BLK_DEV + local_block
        return blocks[jax.random.permutation(key_order, TILES_DEV)]
    return jax.vmap(device_tiles)(jnp.arange(N_DP)).reshape(-1).astype(jnp.int32)


def draw_tile_rows(key, part):
    return tile_blocks(key, 101)


def draw_tile_cols(key, part):
    return tile_blocks(key, 202)


def attention_vector(key):
    key_base = jax.random.fold_in(key, 0)
    vector = 0.25 * jnp.clip(jax.random.normal(key_base, (HEADS, HD), jnp.float32), -4.0, 4.0)
    return vector.reshape(-1)


def draw_att_src(key, part):
    return attention_vector(jax.random.fold_in(key, 11))


def draw_att_dst(key, part):
    return attention_vector(jax.random.fold_in(key, 23))


def plant(entries, key, smallest, top_value):
    index_at = [jax.random.randint(jax.random.fold_in(key, axis), (), 0, length) for axis, length in enumerate(entries.shape)]
    widest = entries.shape.index(max(entries.shape))
    neighbour = index_at[:widest] + [(index_at[widest] + 1) % entries.shape[widest]] + index_at[widest + 1:]
    return entries.at[tuple(index_at)].set(smallest).at[tuple(neighbour)].set(top_value)


def levels(rng, shape, pieces, low, top_value):
    loudness, own = 1.0, jax.random.fold_in(rng, 6)
    for dim, parts in pieces:
        draws = jnp.exp(jax.random.uniform(jax.random.fold_in(own, dim), (parts,), jnp.float32, low / len(pieces), top_value / len(pieces)))
        loudness = loudness * jnp.repeat(draws, shape[dim] // parts).reshape([-1 if axis == dim else 1 for axis in range(len(shape))])
    return loudness


def bell_draw(stream_key, extent, width, limit, shards=(), held_as=jnp.bfloat16):
    values = width * jax.random.normal(stream_key, extent, jnp.float32)
    if shards:
        values = values * levels(stream_key, extent, shards, -0.22, 0.18)
    return jnp.clip(values, -limit, limit).astype(held_as)


def setup_inputs(seed: int = 0) -> dict:
    streams_of = jax.random.split(jax.random.key(seed), 9)
    return {
        "node_feats": bell_draw(streams_of[0], (FIN, NODES), 1.0, 6.0, ((0, 8), (1, 64))),
        "proj_weight": bell_draw(streams_of[1], (HEADS * HD, FIN), FIN ** -0.5, 0.375, ((0, 8),)),
        "att_src": draw_att_src(jax.random.fold_in(streams_of[8], 71), 0),
        "att_dst": draw_att_dst(jax.random.fold_in(streams_of[8], 71), 0),
        "out_bias": bell_draw(streams_of[4], (HEADS * HD,), 0.5, 3.0, ((0, 8),), jnp.float32),
        "tile_rows": draw_tile_rows(jax.random.fold_in(streams_of[8], 71), 0),
        "tile_cols": draw_tile_cols(jax.random.fold_in(streams_of[8], 71), 0),
        "tile_masks": plant(jax.random.randint(streams_of[7], (TILES, TILE // 32, TILE), -2147483648, 2147483647), jax.random.fold_in(streams_of[7], 1), -2147483648, 2147483646).astype(jnp.int32),
    }


far_below = -1.0e30


def leaky_relu(scores):
    return jnp.where(scores > 0, scores, 0.2 * scores)


def unpack_bits(packed):
    offsets = jnp.arange(32, dtype=jnp.int32)
    spread = jnp.bitwise_and(jnp.right_shift(packed[..., :, None, :], offsets[:, None]), 1)
    return spread.reshape(packed.shape[:-2] + (packed.shape[-2] * 32, packed.shape[-1])).astype(jnp.int32)


def edge_scores(edge_mask, source, target):
    raw_scores = leaky_relu(target[:, :, None, :] + source[:, :, :, None])
    return jnp.where(edge_mask[:, None] == 1, raw_scores, far_below)


def reference(node_feats, proj_weight, att_src, att_dst, out_bias, tile_rows, tile_cols, tile_masks):
    projected = jnp.dot(proj_weight, node_feats, preferred_element_type=jnp.float32)
    features = projected.astype(jnp.bfloat16)
    by_head = projected.reshape(HEADS, HD, NODES)
    source = jnp.einsum("hd,hdn->hn", att_src.reshape(HEADS, HD), by_head, precision=lax.Precision.HIGHEST)
    target = jnp.einsum("hd,hdn->hn", att_dst.reshape(HEADS, HD), by_head, precision=lax.Precision.HIGHEST)
    source_blocks = source.reshape(HEADS, NBLK, TILE).transpose(1, 0, 2)
    target_blocks = target.reshape(HEADS, NBLK, TILE).transpose(1, 0, 2)
    feat_blocks = features.reshape(HEADS, HD, NBLK, TILE).transpose(2, 0, 1, 3)
    group_rows = tile_rows.reshape(-1, TILES_DEV)
    group_cols = tile_cols.reshape(-1, TILES_DEV)
    group_masks = tile_masks.reshape(-1, TILES_DEV, TILE // 32, TILE)

    def tile_scores(inputs):
        row_ids, col_ids, packed = inputs
        edge_mask = unpack_bits(packed)
        scores = edge_scores(edge_mask, source_blocks[col_ids], target_blocks[row_ids])
        tile_peaks = jnp.max(scores, axis=2)
        weights = jnp.where(edge_mask[:, None] == 1, jnp.exp(scores - tile_peaks[:, :, None, :]), 0.0)
        return tile_peaks, weights

    def first_pass(inputs):
        tile_peaks, weights = tile_scores(inputs)
        return tile_peaks, jnp.sum(weights, axis=2)

    tile_peaks, masses = lax.map(first_pass, (group_rows, group_cols, group_masks))
    tile_peaks = tile_peaks.reshape(TILES, HEADS, TILE)
    masses = masses.reshape(TILES, HEADS, TILE)
    self_scores = leaky_relu(source_blocks + target_blocks)
    row_peak = self_scores.at[tile_rows].max(tile_peaks)
    self_weight = jnp.exp(self_scores - row_peak)
    denominator = self_weight.at[tile_rows].add(jnp.exp(tile_peaks - row_peak[tile_rows]) * masses)

    def second_pass(summed, inputs):
        row_ids, col_ids, packed = inputs
        peaks_here, weights = tile_scores(inputs)
        rounded = lax.optimization_barrier(weights.astype(jnp.bfloat16)).astype(jnp.float32)
        partial_values = jnp.einsum("ghdc,ghcr->ghdr", feat_blocks[col_ids].astype(jnp.float32), rounded)
        rescale = jnp.exp(peaks_here - row_peak[row_ids])
        return summed.at[row_ids].add(rescale[:, :, None, :] * partial_values), None

    start_sum = self_weight[:, :, None, :] * feat_blocks.astype(jnp.float32)
    summed, ignored = lax.scan(second_pass, start_sum, (group_rows, group_cols, group_masks))
    gathered = summed / denominator[:, :, None, :]
    flat_out = gathered.transpose(1, 2, 0, 3).reshape(HEADS * HD, NODES)
    return jax.nn.elu(flat_out + node_feats.astype(jnp.float32) + out_bias[:, None]).astype(jnp.bfloat16)
```

```python
import functools

import jax
import jax.numpy as jnp
from jax import lax
from jax.experimental import pallas as pl
from jax.experimental.pallas import tpu as pltpu
from jax.sharding import PartitionSpec as P

MESH = pl.DeviceIdType.MESH
HD = 32
LANES = 128
LOG2E = 1.4426950408889634
NEG = -1e30
FLOOR = -1e28
NX, NZ, NC = 4, 8, 2
CAP = 2
UNROLL = 4


def split3(v):
    a = v.astype(jnp.bfloat16)
    r = v - a.astype(jnp.float32)
    b = r.astype(jnp.bfloat16)
    c = (r - b.astype(jnp.float32)).astype(jnp.bfloat16)
    return [t.astype(jnp.float32) for t in (a, b, c)]


def rows_of(parts, height, width):
    at = lax.broadcasted_iota(jnp.int32, (height, width), 0)
    out = jnp.zeros((height, width), jnp.float32)
    for i, part in enumerate(parts):
        out = jnp.where(at == i, part, out)
    return out


def wait_bytes(ref, sem):
    pltpu.make_async_copy(ref, ref, sem).wait()


def prep_kernel(nb, rows_ref, cols_ref, mask_ref, slot_ref, code_ref, taken):
    owners = code_ref.shape[0]
    tiles = mask_ref.shape[0]
    code_ref[...] = jnp.full(code_ref.shape, -1, jnp.int32)

    def clear(i, _):
        taken[i] = 0
        return 0

    lax.fori_loop(0, owners, clear, 0)
    lane = lax.broadcasted_iota(jnp.int32, (1, LANES), 1)

    def place(t, _):
        row = rows_ref[t]
        owner = row // nb
        k = taken[owner]
        taken[owner] = k + 1
        slot_ref[owner, k] = mask_ref[t]
        code = (row % nb) + cols_ref[t] * nb
        code_ref[owner] = jnp.where(lane == k, code, code_ref[owner])
        return 0

    lax.fori_loop(0, tiles, place, 0)


def gather_kernel(
    ny, nb, x_ref, w_ref, asrc_ref, adst_ref, slot_ref, code_ref,
    F, S, T4, M4, I4,
    wl, wa, xr, fs, ss, ts,
    one, rf, s_ring, r_ring, s_q, r_q, s_sib, r_sib, s_sibq, r_sibq,
):
    by = nb // ny
    ndp = NX * NZ * NC
    cols = by * LANES
    wr = wl.shape[0]
    dp = lax.axis_index("dp")
    y = lax.axis_index("mp")
    c = dp % NC
    z = (dp // NC) % NZ
    xx = dp // (NC * NZ)
    (SX, RX, SW, RW, SM, RM, SI, RI, SF, SS, RS, ST, RT, STX, RTX, SMX, RMX, SIX, RIX) = [
        one.at[i] for i in range(19)
    ]

    def dev(x_, z_, c_):
        return (x_ * NZ + z_) * NC + c_

    def send(src, dst, ssem, rsem, where):
        pltpu.make_async_remote_copy(
            src_ref=src, dst_ref=dst, send_sem=ssem, recv_sem=rsem,
            device_id=where, device_id_type=MESH,
        ).start()

    barrier = pltpu.get_barrier_semaphore()
    for d in range(1, ny):
        pl.semaphore_signal(barrier, inc=1, device_id={"mp": lax.rem(y + d, ny)}, device_id_type=MESH)

    def greet(j, _):
        pl.semaphore_signal(barrier, inc=1, device_id={"dp": lax.rem(dp + j, ndp)}, device_id_type=MESH)
        return 0

    lax.fori_loop(1, ndp, greet, 0)

    w = w_ref[...]
    fin = w.shape[1]
    att = rows_of(split3(asrc_ref[...]) + split3(adst_ref[...]), 16, HD).astype(jnp.bfloat16)
    v = jnp.dot(att, w, preferred_element_type=jnp.float32) * LOG2E
    vs = v[0:1] + v[1:2] + v[2:3]
    vd = v[3:4] + v[4:5] + v[5:6]
    wl[0:HD, :] = w
    wl[HD:wr, :] = rows_of(split3(vs) + split3(vd), 16, fin).astype(jnp.bfloat16)
    xr[pl.ds(pl.multiple_of(y * HD, HD), HD), :] = x_ref[:, pl.ds(pl.multiple_of(y * cols, cols), cols)]
    wa[y] = wl[...]
    M4[xx, dp] = slot_ref[dp]
    I4[xx, dp] = code_ref[dp]

    pl.semaphore_wait(barrier, ndp - 1 + ny - 1)

    for d in range(1, ny):
        p = lax.rem(y + d, ny)
        send(
            x_ref.at[:, pl.ds(pl.multiple_of(p * cols, cols), cols)],
            xr.at[pl.ds(pl.multiple_of(y * HD, HD), HD), :],
            SX, RX, {"mp": p},
        )
        send(wl, wa.at[y], SW, RW, {"mp": p})

    def send_slots(j, _):
        q = lax.rem(dp + j, ndp)
        xq = q // (NC * NZ)
        send(slot_ref.at[q], M4.at[xq, dp], SM, RM, {"dp": q})
        send(code_ref.at[q], I4.at[xq, dp], SI, RI, {"dp": q})
        return 0

    lax.fori_loop(1, ndp, send_slots, 0)

    wait_bytes(xr.at[pl.ds(0, (ny - 1) * HD)], RX)
    wait_bytes(wa.at[pl.ds(0, ny - 1)], RW)

    own = z * NC + c

    def project(h):
        out = jnp.dot(wa[h], xr[...], preferred_element_type=jnp.float32)
        feats = out[0:HD].astype(jnp.bfloat16)
        s = out[HD : HD + 1] + out[HD + 1 : HD + 2] + out[HD + 2 : HD + 3]
        t = out[HD + 3 : HD + 4] + out[HD + 4 : HD + 5] + out[HD + 5 : HD + 6]
        return feats, s, t

    for d in range(1, ny):
        h = lax.rem(y + d, ny)
        feats, s, t = project(h)
        for k in range(by):
            at = slice(k * LANES, (k + 1) * LANES)
            fs[h, k] = feats[:, at]
            ss[h, k : k + 1, :] = s[:, at]
            ts[h, k : k + 1, :] = t[:, at]
    feats, s, t = project(y)
    for k in range(by):
        at = slice(k * LANES, (k + 1) * LANES)
        F[own * nb + y * by + k] = feats[:, at]
        S[own, y, k : k + 1, :] = s[:, at]
        T4[xx, y, k : k + 1, :] = t[:, at]

    for d in range(1, ny):
        p = lax.rem(y + d, ny)
        send(fs.at[p], F.at[pl.ds(own * nb + y * by, by)], SF, rf.at[d], {"mp": p})
        send(ss.at[p], S.at[own, y], SS, RS, {"mp": p})
        send(ts.at[p], T4.at[xx, y], ST, RT, {"mp": p})

    up = {"dp": dev(xx, lax.rem(z + 1, NZ), c)}
    down = {"dp": dev(xx, lax.rem(z + NZ - 1, NZ), c)}
    sib = {"dp": dev(xx, z, NC - 1 - c)}
    ways = (up, down)
    last = NZ // 2
    order = sorted(range(ny), key=lambda d: min(d, ny - d))

    def owner_of(way, hop):
        zo = lax.rem(z + NZ - hop, NZ) if way == 0 else lax.rem(z + hop, NZ)
        return zo * NC + c

    def piece(o, d):
        return F.at[pl.ds(o * nb + lax.rem(y + ny - d, ny) * by, by)]

    def goes(way, hop, i):
        return hop < last or (hop == last and (i < ny // 2) == (way == 0))

    for i, d in enumerate(order):
        if d:
            wait_bytes(piece(own, d), rf.at[d])
        for way in range(2):
            if goes(way, 1, i):
                send(piece(own, d), piece(own, d), s_ring.at[way, 0, i], r_ring.at[way, 0, i], ways[way])
    wait_bytes(S.at[0, pl.ds(0, ny - 1)], RS)
    for way in range(2):
        send(S.at[own], S.at[own], s_q.at[way, 0], r_q.at[way, 0], ways[way])
    wait_bytes(T4.at[0, pl.ds(0, ny - 1)], RT)
    for j in range(1, NX):
        send(T4.at[xx], T4.at[xx], STX, RTX, {"dp": dev(lax.rem(xx + j, NX), z, c)})

    def share(o, i):
        at = pl.ds(o * nb, nb)
        send(F.at[at], F.at[at], s_sib.at[i], r_sib.at[i], sib)
        send(S.at[o], S.at[o], s_sibq.at[i], r_sibq.at[i], sib)

    share(own, 0)

    wait_bytes(M4.at[0, pl.ds(0, ndp - 1)], RM)
    wait_bytes(I4.at[0, pl.ds(0, ndp - 1)], RI)
    for j in range(1, NX):
        to = {"dp": dev(lax.rem(xx + j, NX), z, c)}
        send(M4.at[xx], M4.at[xx], SMX, RMX, to)
        send(I4.at[xx], I4.at[xx], SIX, RIX, to)

    for hop in range(1, last + 1):
        for i, d in enumerate(order):
            for way in range(2):
                if goes(way, hop, i):
                    o = owner_of(way, hop)
                    wait_bytes(piece(o, d), r_ring.at[way, hop - 1, i])
                    if goes(way, hop + 1, i):
                        send(piece(o, d), piece(o, d), s_ring.at[way, hop, i], r_ring.at[way, hop, i], ways[way])
        for way in range(2):
            if hop < last or way == 0:
                o = owner_of(way, hop)
                wait_bytes(S.at[o], r_q.at[way, hop - 1])
                if hop + 1 < last or (hop + 1 == last and way == 0):
                    send(S.at[o], S.at[o], s_q.at[way, hop], r_q.at[way, hop], ways[way])
                share(o, 2 * hop - 1 + way)

    other = NC - 1 - c
    for i in range(NZ):
        hop, way = (i + 1) // 2, (i + 1) % 2
        zo = lax.rem(z + NZ - hop, NZ) if way == 0 else lax.rem(z + hop, NZ)
        o = (zo if i else z) * NC + other
        wait_bytes(F.at[pl.ds(o * nb, nb)], r_sib.at[i])
        wait_bytes(S.at[o], r_sibq.at[i])
    wait_bytes(T4.at[pl.ds(0, NX - 1)], RTX)
    wait_bytes(M4.at[pl.ds(0, NX - 1)], RMX)
    wait_bytes(I4.at[pl.ds(0, NX - 1)], RIX)

    wait_bytes(xr.at[pl.ds(0, (ny - 1) * HD)], SX)
    wait_bytes(wa.at[pl.ds(0, ny - 1)], SW)
    wait_bytes(M4.at[0, pl.ds(0, ndp - 1)], SM)
    wait_bytes(I4.at[0, pl.ds(0, ndp - 1)], SI)
    wait_bytes(fs.at[pl.ds(0, ny - 1)], SF)
    wait_bytes(ss.at[pl.ds(0, ny - 1)], SS)
    wait_bytes(ts.at[pl.ds(0, ny - 1)], ST)
    wait_bytes(T4.at[pl.ds(0, NX - 1)], STX)
    wait_bytes(M4.at[pl.ds(0, NX - 1)], SMX)
    wait_bytes(I4.at[pl.ds(0, NX - 1)], SIX)
    for hop in range(0, last):
        for way in range(2):
            for i, d in enumerate(order):
                if goes(way, hop + 1, i):
                    wait_bytes(piece(own, d), s_ring.at[way, hop, i])
            if hop + 1 < last or way == 0:
                wait_bytes(S.at[own], s_q.at[way, hop])
    for i in range(NZ):
        wait_bytes(F.at[pl.ds(0, nb)], s_sib.at[i])
        wait_bytes(S.at[0], s_sibq.at[i])


def tile_kernel(nb, F, S, T, M, I, pv_ref, pms_ref, st, lst, acc, mx, tbl, sem):
    dp = lax.axis_index("dp")
    xx = dp // (NC * NZ)
    ncol = F.shape[0]
    nrow = T.shape[0]
    nslot = M.shape[0]
    nh = I.shape[0]

    code = I[...]
    lane = lax.broadcasted_iota(jnp.int32, code.shape, 1)
    row = lax.broadcasted_iota(jnp.int32, code.shape, 0)
    col = code // nb
    active = (code >= 0) & (lane < CAP) & (col // ncol == xx)
    tri = lax.broadcasted_iota(jnp.int32, (nh, nh), 0) >= lax.broadcasted_iota(jnp.int32, (nh, nh), 1)
    flags = active.astype(jnp.float32)
    rank = jnp.dot(
        tri.astype(jnp.float32).astype(jnp.bfloat16), flags.astype(jnp.bfloat16), preferred_element_type=jnp.float32
    )
    totals = jnp.sum(flags, axis=0, keepdims=True)
    lane0 = lax.broadcasted_iota(jnp.int32, (1, LANES), 1)
    before = [jnp.zeros((1, 1), jnp.float32)]
    for k in range(CAP):
        before.append(before[-1] + jnp.sum(jnp.where(lane0 == k, totals, 0.0), axis=1, keepdims=True))
    entry = (row * CAP + lane) + ((code % nb) + (col % ncol) * nb) * nslot
    entry = jnp.where(active, entry, 0)
    chunks = tbl.shape[0] - 1
    want = lane0 + 1
    got = [jnp.zeros((1, LANES), jnp.int32) for _ in range(chunks)]
    for k in range(CAP):
        r = (rank[:, k : k + 1] + before[k]).astype(jnp.int32)
        e = entry[:, k : k + 1]
        r = jnp.where(active[:, k : k + 1], r, 0)
        for j in range(chunks):
            got[j] = got[j] + jnp.sum(jnp.where(r == want + j * LANES, e, 0), axis=0, keepdims=True)
    for j in range(chunks):
        tbl[j] = got[j]
    tbl[chunks] = jnp.broadcast_to(before[CAP], (1, LANES)).astype(jnp.int32)
    copy = pltpu.make_async_copy(tbl, lst, sem)
    copy.start()

    for j in range(ncol // LANES):
        st[j] = S[j * LANES : (j + 1) * LANES, :].T
    acc[...] = jnp.zeros(acc.shape, jnp.float32)
    mx[...] = jnp.full(mx.shape, FLOOR, jnp.float32)
    copy.wait()
    count = lst[chunks, 0, 0]

    sub = lax.broadcasted_iota(jnp.int32, (8, LANES), 0)
    ones = jnp.where(
        lax.broadcasted_iota(jnp.int32, (16, LANES), 0) == 0, 1.0, 0.0
    ).astype(jnp.bfloat16)

    def one_tile(idx):
        e = lst[idx // LANES, 0, idx % LANES]
        slot = e % nslot
        rest = e // nslot
        rb = rest % nb
        cl = rest // nb
        r = (slot // (nslot // NX)) * nb + rb
        bits = jnp.where(idx < count, M[slot], 0)
        scol = st[cl // LANES]
        t = T[r]
        which = jnp.full((8, LANES), cl % LANES, jnp.int32)
        picked = []
        top = jnp.full((8, LANES), NEG, jnp.float32)
        for g in range(LANES // 8):
            word = jnp.broadcast_to(bits[g // 4 : g // 4 + 1, :], (8, LANES))
            up = lax.shift_left(word, 31 - (8 * (g % 4)) - sub)
            s = jnp.take_along_axis(scol[8 * g : 8 * g + 8, :], which, axis=1)
            s = jnp.where(up < 0, s, NEG)
            top = jnp.maximum(top, s)
            picked.append(s)
        m = jnp.max(top, axis=0, keepdims=True) + t
        ref = jnp.maximum(jnp.maximum(m, 0.2 * m), FLOOR)
        weights = []
        for s in picked:
            u = s + t
            weights.append(jnp.exp2(jnp.maximum(u, 0.2 * u) - ref))
        wts = jnp.concatenate(weights, axis=0).astype(jnp.bfloat16)
        lhs = jnp.concatenate([F[cl], ones], axis=0)
        val = jnp.dot(lhs, wts, preferred_element_type=jnp.float32)
        return r, ref, val[0 : HD + 8]

    def step(it, _):
        found = [one_tile(it * UNROLL + u) for u in range(UNROLL)]
        for r, ref, val in found:
            old = mx[r]
            new = jnp.maximum(old, ref)
            acc[r] = acc[r] * jnp.exp2(old - new) + val * jnp.exp2(ref - new)
            mx[r] = new
        return 0

    lax.fori_loop(0, (count + UNROLL - 1) // UNROLL, step, 0)

    def put(r, _):
        a = acc[r]
        pv_ref[r] = a[0:HD].astype(jnp.bfloat16)
        pms_ref[r, 0:1, :] = mx[r]
        pms_ref[r, 1:2, :] = a[HD : HD + 1]
        return 0

    lax.fori_loop(0, nrow, put, 0)


def merge_kernel(nb, F, S, T4, x_ref, b_ref, pv, pms, out_ref, rv, rms, fo, so, to, loc, s_v, r_v, s_m, r_m):
    dp = lax.axis_index("dp")
    c = dp % NC
    z = (dp // NC) % NZ
    xx = dp // (NC * NZ)
    own = z * NC + c
    by = so.shape[1]
    copies = [
        pltpu.make_async_copy(F.at[pl.ds(own * nb, nb)], fo, loc.at[0]),
        pltpu.make_async_copy(S.at[own], so, loc.at[1]),
        pltpu.make_async_copy(T4.at[xx], to, loc.at[2]),
    ]
    for cp in copies:
        cp.start()
    barrier = pltpu.get_barrier_semaphore()
    peers = [lax.rem(xx + j, NX) for j in range(1, NX)]
    for p in peers:
        pl.semaphore_signal(barrier, inc=1, device_id={"dp": (p * NZ + z) * NC + c}, device_id_type=MESH)
    pl.semaphore_wait(barrier, NX - 1)
    sends = []
    for j, p in enumerate(peers):
        at = {"dp": (p * NZ + z) * NC + c}
        for src, dst, ssem, rsem in ((pms, rms, s_m, r_m), (pv, rv, s_v, r_v)):
            cp = pltpu.make_async_remote_copy(
                src_ref=src.at[p], dst_ref=dst.at[j], send_sem=ssem.at[j], recv_sem=rsem.at[j],
                device_id=at, device_id_type=MESH,
            )
            cp.start()
            sends.append(cp)
    for cp in copies:
        cp.wait()
    rowi = lax.broadcasted_iota(jnp.int32, (HD, LANES), 0)
    lanei = lax.broadcasted_iota(jnp.int32, (HD, LANES), 1)
    bias = jnp.sum(jnp.where(rowi == lanei, b_ref[...], 0.0), axis=1, keepdims=True)
    for cp in sends:
        cp.wait_recv()
    for b in range(nb):
        k = b % by
        s = so[b // by, k : k + 1, :] + to[b // by, k : k + 1, :]
        s = jnp.maximum(s, 0.2 * s)
        parts = [(pms[xx, b], pv[xx, b])] + [(rms[j, b], rv[j, b]) for j in range(NX - 1)]
        best = s
        for pm, _ in parts:
            best = jnp.maximum(best, pm[0:1])
        e = jnp.exp2(s - best)
        den = e
        total = e * fo[b].astype(jnp.float32)
        for pm, val in parts:
            e = jnp.exp2(pm[0:1] - best)
            den = den + e * pm[1:2]
            total = total + e * val.astype(jnp.float32)
        at = slice(b * LANES, (b + 1) * LANES)
        v = total / den + x_ref[:, at].astype(jnp.float32) + bias
        v = jnp.where(v > 0, v, jnp.exp2(jnp.minimum(v, 0.0) * LOG2E) - 1.0)
        out_ref[:, at] = v.astype(jnp.bfloat16)
    for cp in sends:
        cp.wait_send()


def local(node_feats, proj_weight, att_src, att_dst, out_bias, tile_rows, tile_cols, tile_masks):
    n = node_feats.shape[1]
    fin = proj_weight.shape[1]
    ny = fin // HD
    nb = n // LANES
    by = nb // ny
    ndp = NX * NZ * NC
    tiles = tile_rows.shape[0]
    vmem = pl.BlockSpec(memory_space=pltpu.VMEM)
    smem = pl.BlockSpec(memory_space=pltpu.SMEM)
    hbm = pl.BlockSpec(memory_space=pl.ANY)
    f32, i32, bf16 = jnp.float32, jnp.int32, jnp.bfloat16
    shape = jax.ShapeDtypeStruct
    dma = pltpu.SemaphoreType.DMA

    slots, codes = pl.pallas_call(
        functools.partial(prep_kernel, nb),
        out_shape=(shape((ndp, CAP, 4, LANES), i32), shape((ndp, 1, LANES), i32)),
        in_specs=[smem, smem, vmem],
        out_specs=(vmem, vmem),
        scratch_shapes=[pltpu.SMEM((ndp,), i32)],
        name="prep",
    )(tile_rows, tile_cols, tile_masks)

    ng = NZ * NC
    wr = HD + 16
    F, S, T4, M4, I4 = pl.pallas_call(
        functools.partial(gather_kernel, ny, nb),
        out_shape=(
            shape((ng * nb, HD, LANES), bf16),
            shape((ng, ny, by, LANES), f32),
            shape((NX, ny, by, LANES), f32),
            shape((NX, ndp, CAP, 4, LANES), i32),
            shape((NX, ndp, 1, LANES), i32),
        ),
        in_specs=[vmem] * 6,
        out_specs=(vmem,) * 5,
        scratch_shapes=[
            pltpu.VMEM((wr, fin), bf16),
            pltpu.VMEM((ny, wr, fin), bf16),
            pltpu.VMEM((fin, by * LANES), bf16),
            pltpu.VMEM((ny, by, HD, LANES), bf16),
            pltpu.VMEM((ny, by, LANES), f32),
            pltpu.VMEM((ny, by, LANES), f32),
            dma((19,)),
            dma((ny,)),
            dma((2, NZ // 2, ny)),
            dma((2, NZ // 2, ny)),
            dma((2, NZ // 2)),
            dma((2, NZ // 2)),
            dma((NZ,)),
            dma((NZ,)),
            dma((NZ,)),
            dma((NZ,)),
        ],
        compiler_params=pltpu.CompilerParams(collective_id=0, has_side_effects=True),
        name="gather",
    )(node_feats, proj_weight, att_src.reshape(1, HD), att_dst.reshape(1, HD), slots, codes)

    nrow = NX * nb
    nslot = NX * ndp * CAP
    chunks = max(1, nslot // LANES)
    pv, pms = pl.pallas_call(
        functools.partial(tile_kernel, nb),
        out_shape=(shape((nrow, HD, LANES), bf16), shape((nrow, 2, LANES), f32)),
        in_specs=[vmem] * 5,
        out_specs=(vmem, vmem),
        scratch_shapes=[
            pltpu.VMEM((max(1, ng * nb // LANES), LANES, LANES), f32),
            pltpu.SMEM((chunks + 1, 1, LANES), i32),
            pltpu.VMEM((nrow, HD + 8, LANES), f32),
            pltpu.VMEM((nrow, 1, LANES), f32),
            pltpu.VMEM((chunks + 1, 1, LANES), i32),
            dma(()),
        ],
        name="tiles",
    )(
        F,
        S.reshape(ng * nb, LANES),
        T4.reshape(nrow, 1, LANES),
        M4.reshape(nslot, 4, LANES),
        I4.reshape(NX * ndp, LANES),
    )

    return pl.pallas_call(
        functools.partial(merge_kernel, nb),
        out_shape=shape((HD, n), bf16),
        in_specs=[hbm, hbm, hbm, vmem, vmem, vmem, vmem],
        out_specs=vmem,
        scratch_shapes=[
            pltpu.VMEM((NX - 1, nb, HD, LANES), bf16),
            pltpu.VMEM((NX - 1, nb, 2, LANES), f32),
            pltpu.VMEM((nb, HD, LANES), bf16),
            pltpu.VMEM((ny, by, LANES), f32),
            pltpu.VMEM((ny, by, LANES), f32),
            dma((3,)),
            dma((NX - 1,)),
            dma((NX - 1,)),
            dma((NX - 1,)),
            dma((NX - 1,)),
        ],
        compiler_params=pltpu.CompilerParams(collective_id=1, has_side_effects=True),
        name="merge",
    )(
        F, S, T4, node_feats,
        jnp.pad(out_bias, (0, LANES - HD)).reshape(1, LANES),
        pv.reshape(NX, nb, HD, LANES),
        pms.reshape(NX, nb, 2, LANES),
    )


def solution(mesh):
    return jax.shard_map(
        local,
        mesh=mesh,
        in_specs=(
            P("mp", "dp"),
            P("mp", None),
            P("mp"),
            P("mp"),
            P("mp"),
            P("dp"),
            P("dp"),
            P("dp", None, None),
        ),
        out_specs=P("mp", "dp"),
        check_vma=False,
    )
```

```python
import functools

import jax
import jax.numpy as jnp
from jax import lax
from jax.experimental import pallas as pl
from jax.experimental.pallas import tpu as pltpu
from jax.sharding import PartitionSpec as P

MESH = pl.DeviceIdType.MESH
HD = 32
LANES = 128
LOG2E = 1.4426950408889634
NEG = -1e30
FLOOR = -1e28
NX, NZ, NC = 4, 8, 2
CAP = 2
UNROLL = 4
ROOM = 24 * 2**20


def split3(v):
    a = v.astype(jnp.bfloat16)
    r = v - a.astype(jnp.float32)
    b = r.astype(jnp.bfloat16)
    c = (r - b.astype(jnp.float32)).astype(jnp.bfloat16)
    return [t.astype(jnp.float32) for t in (a, b, c)]


def rows_of(parts, height, width):
    at = lax.broadcasted_iota(jnp.int32, (height, width), 0)
    out = jnp.zeros((height, width), jnp.float32)
    for i, part in enumerate(parts):
        out = jnp.where(at == i, part, out)
    return out


def on_chip(shape, dtype):
    return pltpu.VMEM(shape, dtype)


def held(x):
    return pltpu.with_memory_space_constraint(x, pltpu.VMEM)


def wait_bytes(ref, sem):
    pltpu.make_async_copy(ref, ref, sem).wait()


def prep_kernel(nb, rows_ref, cols_ref, mask_ref, slot_ref, code_ref, taken):
    owners = code_ref.shape[0]
    tiles = mask_ref.shape[0]
    code_ref[...] = jnp.full(code_ref.shape, -1, jnp.int32)

    def clear(i, _):
        taken[i] = 0
        return 0

    lax.fori_loop(0, owners, clear, 0)
    lane = lax.broadcasted_iota(jnp.int32, (1, LANES), 1)

    def place(t, _):
        row = rows_ref[t]
        owner = row // nb
        k = taken[owner]
        taken[owner] = k + 1
        slot_ref[owner, k] = mask_ref[t]
        code = (row % nb) + cols_ref[t] * nb
        code_ref[owner] = jnp.where(lane == k, code, code_ref[owner])
        return 0

    lax.fori_loop(0, tiles, place, 0)


def gather_kernel(
    ny, nb, x_ref, w_ref, asrc_ref, adst_ref, slot_ref, code_ref,
    F, S, T4, M4, I4,
    wl, wa, xr, fs, ss, ts,
    one, rf, s_ring, r_ring, s_q, r_q, s_sib, r_sib, s_sibq, r_sibq,
):
    by = nb // ny
    ndp = NX * NZ * NC
    cols = by * LANES
    wr = wl.shape[0]
    dp = lax.axis_index("dp")
    y = lax.axis_index("mp")
    c = dp % NC
    z = (dp // NC) % NZ
    xx = dp // (NC * NZ)
    (SX, RX, SW, RW, SM, RM, SI, RI, SF, SS, RS, ST, RT, STX, RTX, SMX, RMX, SIX, RIX) = [
        one.at[i] for i in range(19)
    ]

    def dev(x_, z_, c_):
        return (x_ * NZ + z_) * NC + c_

    def send(src, dst, ssem, rsem, where):
        pltpu.make_async_remote_copy(
            src_ref=src, dst_ref=dst, send_sem=ssem, recv_sem=rsem,
            device_id=where, device_id_type=MESH,
        ).start()

    barrier = pltpu.get_barrier_semaphore()
    for d in range(1, ny):
        pl.semaphore_signal(barrier, inc=1, device_id={"mp": lax.rem(y + d, ny)}, device_id_type=MESH)

    def greet(j, _):
        pl.semaphore_signal(barrier, inc=1, device_id={"dp": lax.rem(dp + j, ndp)}, device_id_type=MESH)
        return 0

    lax.fori_loop(1, ndp, greet, 0)

    w = w_ref[...]
    fin = w.shape[1]
    att = rows_of(split3(asrc_ref[...]) + split3(adst_ref[...]), 16, HD).astype(jnp.bfloat16)
    v = jnp.dot(att, w, preferred_element_type=jnp.float32) * LOG2E
    vs = v[0:1] + v[1:2] + v[2:3]
    vd = v[3:4] + v[4:5] + v[5:6]
    wl[0:HD, :] = w
    wl[HD:wr, :] = rows_of(split3(vs) + split3(vd), 16, fin).astype(jnp.bfloat16)
    xr[pl.ds(pl.multiple_of(y * HD, HD), HD), :] = x_ref[:, pl.ds(pl.multiple_of(y * cols, cols), cols)]
    wa[y] = wl[...]
    M4[xx, dp] = slot_ref[dp]
    I4[xx, dp] = code_ref[dp]

    pl.semaphore_wait(barrier, ndp - 1 + ny - 1)

    for d in range(1, ny):
        p = lax.rem(y + d, ny)
        send(
            x_ref.at[:, pl.ds(pl.multiple_of(p * cols, cols), cols)],
            xr.at[pl.ds(pl.multiple_of(y * HD, HD), HD), :],
            SX, RX, {"mp": p},
        )
        send(wl, wa.at[y], SW, RW, {"mp": p})

    def send_slots(j, _):
        q = lax.rem(dp + j, ndp)
        xq = q // (NC * NZ)
        send(slot_ref.at[q], M4.at[xq, dp], SM, RM, {"dp": q})
        send(code_ref.at[q], I4.at[xq, dp], SI, RI, {"dp": q})
        return 0

    lax.fori_loop(1, ndp, send_slots, 0)

    wait_bytes(xr.at[pl.ds(0, (ny - 1) * HD)], RX)
    wait_bytes(wa.at[pl.ds(0, ny - 1)], RW)

    own = z * NC + c

    def project(h):
        out = jnp.dot(wa[h], xr[...], preferred_element_type=jnp.float32)
        feats = out[0:HD].astype(jnp.bfloat16)
        s = out[HD : HD + 1] + out[HD + 1 : HD + 2] + out[HD + 2 : HD + 3]
        t = out[HD + 3 : HD + 4] + out[HD + 4 : HD + 5] + out[HD + 5 : HD + 6]
        return feats, s, t

    for d in range(1, ny):
        h = lax.rem(y + d, ny)
        feats, s, t = project(h)
        for k in range(by):
            at = slice(k * LANES, (k + 1) * LANES)
            fs[h, k] = feats[:, at]
            ss[h, k : k + 1, :] = s[:, at]
            ts[h, k : k + 1, :] = t[:, at]
    feats, s, t = project(y)
    for k in range(by):
        at = slice(k * LANES, (k + 1) * LANES)
        F[own * nb + y * by + k] = feats[:, at]
        S[own, y, k : k + 1, :] = s[:, at]
        T4[xx, y, k : k + 1, :] = t[:, at]

    for d in range(1, ny):
        p = lax.rem(y + d, ny)
        send(fs.at[p], F.at[pl.ds(own * nb + y * by, by)], SF, rf.at[d], {"mp": p})
        send(ss.at[p], S.at[own, y], SS, RS, {"mp": p})
        send(ts.at[p], T4.at[xx, y], ST, RT, {"mp": p})

    up = {"dp": dev(xx, lax.rem(z + 1, NZ), c)}
    down = {"dp": dev(xx, lax.rem(z + NZ - 1, NZ), c)}
    sib = {"dp": dev(xx, z, NC - 1 - c)}
    ways = (up, down)
    last = NZ // 2
    order = sorted(range(ny), key=lambda d: min(d, ny - d))

    def owner_of(way, hop):
        zo = lax.rem(z + NZ - hop, NZ) if way == 0 else lax.rem(z + hop, NZ)
        return zo * NC + c

    def piece(o, d):
        return F.at[pl.ds(o * nb + lax.rem(y + ny - d, ny) * by, by)]

    def goes(way, hop, i):
        return hop < last or (hop == last and (i < ny // 2) == (way == 0))

    for i, d in enumerate(order):
        if d:
            wait_bytes(piece(own, d), rf.at[d])
        for way in range(2):
            if goes(way, 1, i):
                send(piece(own, d), piece(own, d), s_ring.at[way, 0, i], r_ring.at[way, 0, i], ways[way])
    wait_bytes(S.at[0, pl.ds(0, ny - 1)], RS)
    for way in range(2):
        send(S.at[own], S.at[own], s_q.at[way, 0], r_q.at[way, 0], ways[way])
    wait_bytes(T4.at[0, pl.ds(0, ny - 1)], RT)
    for j in range(1, NX):
        send(T4.at[xx], T4.at[xx], STX, RTX, {"dp": dev(lax.rem(xx + j, NX), z, c)})

    def share(o, i):
        at = pl.ds(o * nb, nb)
        send(F.at[at], F.at[at], s_sib.at[i], r_sib.at[i], sib)
        send(S.at[o], S.at[o], s_sibq.at[i], r_sibq.at[i], sib)

    share(own, 0)

    wait_bytes(M4.at[0, pl.ds(0, ndp - 1)], RM)
    wait_bytes(I4.at[0, pl.ds(0, ndp - 1)], RI)
    for j in range(1, NX):
        to = {"dp": dev(lax.rem(xx + j, NX), z, c)}
        send(M4.at[xx], M4.at[xx], SMX, RMX, to)
        send(I4.at[xx], I4.at[xx], SIX, RIX, to)

    for hop in range(1, last + 1):
        for i, d in enumerate(order):
            for way in range(2):
                if goes(way, hop, i):
                    o = owner_of(way, hop)
                    wait_bytes(piece(o, d), r_ring.at[way, hop - 1, i])
                    if goes(way, hop + 1, i):
                        send(piece(o, d), piece(o, d), s_ring.at[way, hop, i], r_ring.at[way, hop, i], ways[way])
        for way in range(2):
            if hop < last or way == 0:
                o = owner_of(way, hop)
                wait_bytes(S.at[o], r_q.at[way, hop - 1])
                if hop + 1 < last or (hop + 1 == last and way == 0):
                    send(S.at[o], S.at[o], s_q.at[way, hop], r_q.at[way, hop], ways[way])
                share(o, 2 * hop - 1 + way)

    other = NC - 1 - c
    for i in range(NZ):
        hop, way = (i + 1) // 2, (i + 1) % 2
        zo = lax.rem(z + NZ - hop, NZ) if way == 0 else lax.rem(z + hop, NZ)
        o = (zo if i else z) * NC + other
        wait_bytes(F.at[pl.ds(o * nb, nb)], r_sib.at[i])
        wait_bytes(S.at[o], r_sibq.at[i])
    wait_bytes(T4.at[pl.ds(0, NX - 1)], RTX)
    wait_bytes(M4.at[pl.ds(0, NX - 1)], RMX)
    wait_bytes(I4.at[pl.ds(0, NX - 1)], RIX)

    wait_bytes(xr.at[pl.ds(0, (ny - 1) * HD)], SX)
    wait_bytes(wa.at[pl.ds(0, ny - 1)], SW)
    wait_bytes(M4.at[0, pl.ds(0, ndp - 1)], SM)
    wait_bytes(I4.at[0, pl.ds(0, ndp - 1)], SI)
    wait_bytes(fs.at[pl.ds(0, ny - 1)], SF)
    wait_bytes(ss.at[pl.ds(0, ny - 1)], SS)
    wait_bytes(ts.at[pl.ds(0, ny - 1)], ST)
    wait_bytes(T4.at[pl.ds(0, NX - 1)], STX)
    wait_bytes(M4.at[pl.ds(0, NX - 1)], SMX)
    wait_bytes(I4.at[pl.ds(0, NX - 1)], SIX)
    for hop in range(0, last):
        for way in range(2):
            for i, d in enumerate(order):
                if goes(way, hop + 1, i):
                    wait_bytes(piece(own, d), s_ring.at[way, hop, i])
            if hop + 1 < last or way == 0:
                wait_bytes(S.at[own], s_q.at[way, hop])
    for i in range(NZ):
        wait_bytes(F.at[pl.ds(0, nb)], s_sib.at[i])
        wait_bytes(S.at[0], s_sibq.at[i])


def tile_kernel(nb, F, S, T, M, I, pv_ref, pms_ref, st, lst, acc, mx, tbl, sem):
    dp = lax.axis_index("dp")
    xx = dp // (NC * NZ)
    ncol = F.shape[0]
    nrow = T.shape[0]
    nslot = M.shape[0]
    nh = I.shape[0]

    code = I[...]
    lane = lax.broadcasted_iota(jnp.int32, code.shape, 1)
    row = lax.broadcasted_iota(jnp.int32, code.shape, 0)
    col = code // nb
    active = (code >= 0) & (lane < CAP) & (col // ncol == xx)
    tri = lax.broadcasted_iota(jnp.int32, (nh, nh), 0) >= lax.broadcasted_iota(jnp.int32, (nh, nh), 1)
    flags = active.astype(jnp.float32)
    rank = jnp.dot(
        tri.astype(jnp.float32).astype(jnp.bfloat16), flags.astype(jnp.bfloat16), preferred_element_type=jnp.float32
    )
    totals = jnp.sum(flags, axis=0, keepdims=True)
    lane0 = lax.broadcasted_iota(jnp.int32, (1, LANES), 1)
    before = [jnp.zeros((1, 1), jnp.float32)]
    for k in range(CAP):
        before.append(before[-1] + jnp.sum(jnp.where(lane0 == k, totals, 0.0), axis=1, keepdims=True))
    entry = (row * CAP + lane) + ((code % nb) + (col % ncol) * nb) * nslot
    entry = jnp.where(active, entry, 0)
    chunks = tbl.shape[0] - 1
    want = lane0 + 1
    got = [jnp.zeros((1, LANES), jnp.int32) for _ in range(chunks)]
    for k in range(CAP):
        r = (rank[:, k : k + 1] + before[k]).astype(jnp.int32)
        e = entry[:, k : k + 1]
        r = jnp.where(active[:, k : k + 1], r, 0)
        for j in range(chunks):
            got[j] = got[j] + jnp.sum(jnp.where(r == want + j * LANES, e, 0), axis=0, keepdims=True)
    for j in range(chunks):
        tbl[j] = got[j]
    tbl[chunks] = jnp.broadcast_to(before[CAP], (1, LANES)).astype(jnp.int32)
    copy = pltpu.make_async_copy(tbl, lst, sem)
    copy.start()

    for j in range(ncol // LANES):
        st[j] = S[j * LANES : (j + 1) * LANES, :].T
    acc[...] = jnp.zeros(acc.shape, jnp.float32)
    mx[...] = jnp.full(mx.shape, FLOOR, jnp.float32)
    copy.wait()
    count = lst[chunks, 0, 0]

    sub = lax.broadcasted_iota(jnp.int32, (8, LANES), 0)
    ones = jnp.where(
        lax.broadcasted_iota(jnp.int32, (16, LANES), 0) == 0, 1.0, 0.0
    ).astype(jnp.bfloat16)

    def one_tile(idx):
        e = lst[idx // LANES, 0, idx % LANES]
        slot = e % nslot
        rest = e // nslot
        rb = rest % nb
        cl = rest // nb
        r = (slot // (nslot // NX)) * nb + rb
        bits = jnp.where(idx < count, M[slot], 0)
        scol = st[cl // LANES]
        t = T[r]
        which = jnp.full((8, LANES), cl % LANES, jnp.int32)
        picked = []
        top = jnp.full((8, LANES), NEG, jnp.float32)
        for g in range(LANES // 8):
            word = jnp.broadcast_to(bits[g // 4 : g // 4 + 1, :], (8, LANES))
            up = lax.shift_left(word, 31 - (8 * (g % 4)) - sub)
            s = jnp.take_along_axis(scol[8 * g : 8 * g + 8, :], which, axis=1)
            s = jnp.where(up < 0, s, NEG)
            top = jnp.maximum(top, s)
            picked.append(s)
        m = jnp.max(top, axis=0, keepdims=True) + t
        ref = jnp.maximum(jnp.maximum(m, 0.2 * m), FLOOR)
        weights = []
        for s in picked:
            u = s + t
            weights.append(jnp.exp2(jnp.maximum(u, 0.2 * u) - ref))
        wts = jnp.concatenate(weights, axis=0).astype(jnp.bfloat16)
        lhs = jnp.concatenate([F[cl], ones], axis=0)
        val = jnp.dot(lhs, wts, preferred_element_type=jnp.float32)
        return r, ref, val[0 : HD + 8]

    def step(it, _):
        found = [one_tile(it * UNROLL + u) for u in range(UNROLL)]
        for r, ref, val in found:
            old = mx[r]
            new = jnp.maximum(old, ref)
            acc[r] = acc[r] * jnp.exp2(old - new) + val * jnp.exp2(ref - new)
            mx[r] = new
        return 0

    lax.fori_loop(0, (count + UNROLL - 1) // UNROLL, step, 0)

    def put(r, _):
        a = acc[r]
        pv_ref[r] = a[0:HD].astype(jnp.bfloat16)
        pms_ref[r, 0:1, :] = mx[r]
        pms_ref[r, 1:2, :] = a[HD : HD + 1]
        return 0

    lax.fori_loop(0, nrow, put, 0)


def merge_kernel(
    nb, F, S, T4, x_ref, b_ref, pv, pms, out_ref,
    rv, rms, hv, hms, total_ref, state_ref, s_v, r_v, s_m, r_m,
):
    dp = lax.axis_index("dp")
    c = dp % NC
    z = (dp // NC) % NZ
    xx = dp // (NC * NZ)
    own = z * NC + c
    by = S.shape[2]
    half = nb // 2
    up, opp, down = [lax.rem(xx + j, NX) for j in (1, 2, 3)]

    def dev(p):
        return {"dp": (p * NZ + z) * NC + c}

    barrier = pltpu.get_barrier_semaphore()
    for p in (up, down):
        pl.semaphore_signal(barrier, inc=1, device_id=dev(p), device_id_type=MESH)
    pl.semaphore_wait(barrier, 2)

    def both(i, src_v, dst_v, src_m, dst_m, p):
        out = []
        for src, dst, ssem, rsem in ((src_m, dst_m, s_m, r_m), (src_v, dst_v, s_v, r_v)):
            cp = pltpu.make_async_remote_copy(
                src_ref=src, dst_ref=dst, send_sem=ssem.at[i], recv_sem=rsem.at[i],
                device_id=dev(p), device_id_type=MESH,
            )
            cp.start()
            out.append(cp)
        return out

    lo, hi = pl.ds(0, half), pl.ds(half, half)
    via_up = both(0, pv.at[opp, lo], hv.at[0], pms.at[opp, lo], hms.at[0], up)
    via_down = both(1, pv.at[opp, hi], hv.at[1], pms.at[opp, hi], hms.at[1], down)
    to_up = both(2, pv.at[up], rv.at[0], pms.at[up], rms.at[0], up)
    to_down = both(3, pv.at[down], rv.at[1], pms.at[down], rms.at[1], down)

    rowi = lax.broadcasted_iota(jnp.int32, (HD, HD), 0)
    lanei = lax.broadcasted_iota(jnp.int32, (HD, HD), 1)
    bias = jnp.sum(jnp.where(rowi == lanei, b_ref[...], 0.0), axis=1, keepdims=True)

    for cp in via_up:
        cp.wait_recv()
    on_up = both(4, hv.at[0], rv.at[2, lo], hms.at[0], rms.at[2, lo], up)
    for cp in via_down:
        cp.wait_recv()
    on_down = both(5, hv.at[1], rv.at[2, hi], hms.at[1], rms.at[2, hi], down)
    for cp in to_up + to_down:
        cp.wait_recv()

    def join(best, den, total, pm, val):
        new = jnp.maximum(best, pm[0:1])
        old_e = jnp.exp2(best - new)
        e = jnp.exp2(pm[0:1] - new)
        return new, den * old_e + e * pm[1:2], total * old_e + e * val.astype(jnp.float32)

    for b in range(nb):
        k = b % by
        s = S[own, b // by, k : k + 1, :] + T4[xx, b // by, k : k + 1, :]
        best = jnp.maximum(s, 0.2 * s)
        den = jnp.ones_like(best)
        total = F[own * nb + b].astype(jnp.float32)
        for pm, val in ((pms[xx, b], pv[xx, b]), (rms[0, b], rv[0, b]), (rms[1, b], rv[1, b])):
            best, den, total = join(best, den, total, pm, val)
        total_ref[b] = total
        state_ref[b, 0:1, :] = best
        state_ref[b, 1:2, :] = den
    for cp in on_up + on_down:
        cp.wait_recv()
    for b in range(nb):
        best, den, total = join(state_ref[b, 0:1, :], state_ref[b, 1:2, :], total_ref[b], rms[2, b], rv[2, b])
        at = slice(b * LANES, (b + 1) * LANES)
        v = total / den + x_ref[:, at].astype(jnp.float32) + bias
        v = jnp.where(v > 0, v, jnp.exp2(jnp.minimum(v, 0.0) * LOG2E) - 1.0)
        out_ref[:, at] = v.astype(jnp.bfloat16)
    for cp in via_up + via_down + to_up + to_down + on_up + on_down:
        cp.wait_send()


def local(node_feats, proj_weight, att_src, att_dst, out_bias, tile_rows, tile_cols, tile_masks):
    n = node_feats.shape[1]
    fin = proj_weight.shape[1]
    ny = fin // HD
    nb = n // LANES
    by = nb // ny
    ndp = NX * NZ * NC
    tiles = tile_rows.shape[0]
    vmem = pl.BlockSpec(memory_space=pltpu.VMEM)
    smem = pl.BlockSpec(memory_space=pltpu.SMEM)
    f32, i32, bf16 = jnp.float32, jnp.int32, jnp.bfloat16
    shape = jax.ShapeDtypeStruct
    dma = pltpu.SemaphoreType.DMA

    slots, codes = pl.pallas_call(
        functools.partial(prep_kernel, nb),
        out_shape=(on_chip((ndp, CAP, 4, LANES), i32), on_chip((ndp, 1, LANES), i32)),
        in_specs=[smem, smem, vmem],
        out_specs=(vmem, vmem),
        scratch_shapes=[pltpu.SMEM((ndp,), i32)],
        compiler_params=pltpu.CompilerParams(vmem_limit_bytes=ROOM),
        name="prep",
    )(tile_rows, tile_cols, tile_masks)

    ng = NZ * NC
    wr = HD + 16
    F, S, T4, M4, I4 = pl.pallas_call(
        functools.partial(gather_kernel, ny, nb),
        out_shape=(
            on_chip((ng * nb, HD, LANES), bf16),
            on_chip((ng, ny, by, LANES), f32),
            on_chip((NX, ny, by, LANES), f32),
            on_chip((NX, ndp, CAP, 4, LANES), i32),
            on_chip((NX, ndp, 1, LANES), i32),
        ),
        in_specs=[vmem] * 6,
        out_specs=(vmem,) * 5,
        scratch_shapes=[
            pltpu.VMEM((wr, fin), bf16),
            pltpu.VMEM((ny, wr, fin), bf16),
            pltpu.VMEM((fin, by * LANES), bf16),
            pltpu.VMEM((ny, by, HD, LANES), bf16),
            pltpu.VMEM((ny, by, LANES), f32),
            pltpu.VMEM((ny, by, LANES), f32),
            dma((19,)),
            dma((ny,)),
            dma((2, NZ // 2, ny)),
            dma((2, NZ // 2, ny)),
            dma((2, NZ // 2)),
            dma((2, NZ // 2)),
            dma((NZ,)),
            dma((NZ,)),
            dma((NZ,)),
            dma((NZ,)),
        ],
        compiler_params=pltpu.CompilerParams(collective_id=0, has_side_effects=True, vmem_limit_bytes=ROOM),
        name="gather",
    )(node_feats, proj_weight, att_src.reshape(1, HD), att_dst.reshape(1, HD), held(slots), held(codes))

    nrow = NX * nb
    nslot = NX * ndp * CAP
    chunks = max(1, nslot // LANES)
    pv, pms = pl.pallas_call(
        functools.partial(tile_kernel, nb),
        out_shape=(on_chip((nrow, HD, LANES), bf16), on_chip((nrow, 2, LANES), f32)),
        in_specs=[vmem] * 5,
        out_specs=(vmem, vmem),
        scratch_shapes=[
            pltpu.VMEM((max(1, ng * nb // LANES), LANES, LANES), f32),
            pltpu.SMEM((chunks + 1, 1, LANES), i32),
            pltpu.VMEM((nrow, HD + 8, LANES), f32),
            pltpu.VMEM((nrow, 1, LANES), f32),
            pltpu.VMEM((chunks + 1, 1, LANES), i32),
            dma(()),
        ],
        compiler_params=pltpu.CompilerParams(vmem_limit_bytes=ROOM),
        name="tiles",
    )(
        held(F),
        held(S.reshape(ng * nb, LANES)),
        held(T4.reshape(nrow, 1, LANES)),
        held(M4.reshape(nslot, 4, LANES)),
        held(I4.reshape(NX * ndp, LANES)),
    )

    return pl.pallas_call(
        functools.partial(merge_kernel, nb),
        out_shape=on_chip((HD, n), bf16),
        in_specs=[vmem] * 7,
        out_specs=vmem,
        scratch_shapes=[
            pltpu.VMEM((3, nb, HD, LANES), bf16),
            pltpu.VMEM((3, nb, 2, LANES), f32),
            pltpu.VMEM((2, nb // 2, HD, LANES), bf16),
            pltpu.VMEM((2, nb // 2, 2, LANES), f32),
            pltpu.VMEM((nb, HD, LANES), f32),
            pltpu.VMEM((nb, 2, LANES), f32),
            dma((6,)),
            dma((6,)),
            dma((6,)),
            dma((6,)),
        ],
        compiler_params=pltpu.CompilerParams(collective_id=1, has_side_effects=True, vmem_limit_bytes=ROOM),
        name="merge",
    )(
        held(F), held(S), held(T4), node_feats, out_bias.reshape(1, HD),
        held(pv.reshape(NX, nb, HD, LANES)),
        held(pms.reshape(NX, nb, 2, LANES)),
    )


def solution(mesh):
    return jax.shard_map(
        local,
        mesh=mesh,
        in_specs=(
            P("mp", "dp"),
            P("mp", None),
            P("mp"),
            P("mp"),
            P("mp"),
            P("dp"),
            P("dp"),
            P("dp", None, None),
        ),
        out_specs=P("mp", "dp"),
        check_vma=False,
    )
```
